16 devices in a mesh: ep: 4 (over z, y), dp: 4 (over x, core).
Axes of the slice: x: 2, y: 2, z: 2, core: 2. Of those that a mesh axis runs over, the one named last changes fastest.
Arguments:
- act_in: bfloat16 [16384, 512], P(('ep', 'dp'))
- grad_out: bfloat16 [16384, 512], P(('ep', 'dp'))
- slot_ids: int32 [2, 16384, 6], P(None, ('ep', 'dp'))
- gate_vals: float32 [2, 16384, 6], P(None, ('ep', 'dp'))
- w_dense: bfloat16 [2, 512, 512], replicated
- w_gate: bfloat16 [2, 64, 512, 352], P(None, 'ep')
- w_up: bfloat16 [2, 64, 512, 352], P(None, 'ep')
- w_down: bfloat16 [2, 64, 352, 512], P(None, 'ep')
- ws_gate: bfloat16 [2, 512, 704], replicated
- ws_up: bfloat16 [2, 512, 704], replicated
- ws_down: bfloat16 [2, 704, 512], replicated
Outputs:
- output 1: bfloat16 [16384, 512], P(('ep', 'dp'))
- output 2: bfloat16 [2, 512, 512], replicated
- output 3: bfloat16 [2, 64, 512, 352], P(None, 'ep')
- output 4: bfloat16 [2, 64, 512, 352], P(None, 'ep')
- output 5: bfloat16 [2, 64, 352, 512], P(None, 'ep')
- output 6: bfloat16 [2, 512, 704], replicated
- output 7: bfloat16 [2, 512, 704], replicated
- output 8: bfloat16 [2, 704, 512], replicated
All inputs are finite; a program needn't handle non-finite values.
Results may differ from the reference program's by a relative error of at most 0.02.
Values are sent between devices in bfloat16 or wider.
A program may use at most 1 GiB of HBM per device.

```python
import functools
import jax
import jax.numpy as jnp
from jax import lax

D = 512
FF = 352
FS = 704
EXPERTS = 64
TOP = 6
TOKENS = 1024
EP = 4
DP = 4
LAYERS = 2

NUM_DEV = EP * DP
CAP = 2 * TOKENS * TOP // EXPERTS
ROWS = NUM_DEV * TOKENS


def draw_slots(key):
    key_tok, key_exp = jax.random.split(key)
    mean_load = TOKENS * TOP // EXPERTS
    order = jax.random.permutation(key_tok, TOKENS)
    position = jnp.arange(TOP, dtype=jnp.int32)[None, :] * TOKENS + order[:, None]
    group = position // (4 * mean_load)
    rest = position % (4 * mean_load)
    first = 2 * mean_load
    second = first + mean_load // 2
    third = second + mean_load // 2
    within = (rest >= first).astype(jnp.int32) + (rest >= second).astype(jnp.int32) + (rest >= third).astype(jnp.int32)
    start = jnp.where(rest >= third, third, jnp.where(rest >= second, second, jnp.where(rest >= first, first, 0)))
    expert_perm = jax.random.permutation(key_exp, EXPERTS)
    expert = expert_perm[group * 4 + within]
    return (expert * CAP + rest - start).astype(jnp.int32)


def setup_inputs(seed: int = 0) -> dict:
    keys = jax.random.split(jax.random.key(seed), 12)
    slot_keys = jax.random.split(keys[0], LAYERS * NUM_DEV)
    slot_ids = jax.vmap(draw_slots)(slot_keys).reshape(LAYERS, ROWS, TOP)
    gate_vals = jax.random.uniform(keys[1], (LAYERS, ROWS, TOP), jnp.float32, 0.5, 1.5) / TOP
    act_in = jax.random.normal(keys[2], (ROWS, D), jnp.float32).astype(jnp.bfloat16)
    grad_out = jax.random.normal(keys[3], (ROWS, D), jnp.float32).astype(jnp.bfloat16)
    w_dense = (jax.random.normal(keys[4], (LAYERS, D, D), jnp.float32) * D ** -0.5).astype(jnp.bfloat16)
    w_gate = (jax.random.normal(keys[5], (LAYERS, EXPERTS, D, FF), jnp.float32) * D ** -0.5).astype(jnp.bfloat16)
    w_up = (jax.random.normal(keys[6], (LAYERS, EXPERTS, D, FF), jnp.float32) * D ** -0.5).astype(jnp.bfloat16)
    w_down = (jax.random.normal(keys[7], (LAYERS, EXPERTS, FF, D), jnp.float32) * FF ** -0.5).astype(jnp.bfloat16)
    ws_gate = (jax.random.normal(keys[8], (LAYERS, D, FS), jnp.float32) * D ** -0.5).astype(jnp.bfloat16)
    ws_up = (jax.random.normal(keys[9], (LAYERS, D, FS), jnp.float32) * D ** -0.5).astype(jnp.bfloat16)
    ws_down = (jax.random.normal(keys[10], (LAYERS, FS, D), jnp.float32) * FS ** -0.5).astype(jnp.bfloat16)
    return {"act_in": act_in, "grad_out": grad_out, "slot_ids": slot_ids, "gate_vals": gate_vals, "w_dense": w_dense, "w_gate": w_gate, "w_up": w_up, "w_down": w_down, "ws_gate": ws_gate, "ws_up": ws_up, "ws_down": ws_down}


def expert_block(args, w_gate32, w_up32, w_down32):
    mixed_loc, slot_loc, gate_loc = args
    slot_flat = slot_loc.reshape(TOKENS * TOP)
    copies = jnp.broadcast_to(mixed_loc[:, None, :], (TOKENS, TOP, D)).reshape(TOKENS * TOP, D)
    dispatched = jnp.zeros((EXPERTS * CAP, D), mixed_loc.dtype).at[slot_flat].set(copies)
    dispatched = dispatched.reshape(EXPERTS, CAP, D).astype(jnp.float32)
    a_one = jnp.einsum("ecd,edf->ecf", dispatched, w_gate32)
    a_three = jnp.einsum("ecd,edf->ecf", dispatched, w_up32)
    hidden = (jax.nn.silu(a_one) * a_three).astype(jnp.bfloat16)
    exp_out = jnp.einsum("ecf,efd->ecd", hidden.astype(jnp.float32), w_down32).astype(jnp.bfloat16)
    picked = exp_out.reshape(EXPERTS * CAP, D)[slot_flat].reshape(TOKENS, TOP, D)
    return jnp.sum(gate_loc[:, :, None] * picked.astype(jnp.float32), axis=1)


def moe_layer(act, layer_in):
    w_dense, w_gate, w_up, w_down, ws_gate, ws_up, ws_down, slot_ids, gate_vals = layer_in
    dense_pre = jnp.dot(act, w_dense, preferred_element_type=jnp.float32)
    mixed = (act.astype(jnp.float32) + dense_pre).astype(jnp.bfloat16)
    s_one = jnp.dot(mixed, ws_gate, preferred_element_type=jnp.float32)
    s_three = jnp.dot(mixed, ws_up, preferred_element_type=jnp.float32)
    shared_hidden = (jax.nn.silu(s_one) * s_three).astype(jnp.bfloat16)
    shared_out = jnp.dot(shared_hidden, ws_down, preferred_element_type=jnp.float32)
    block = jax.checkpoint(functools.partial(expert_block, w_gate32=w_gate.astype(jnp.float32), w_up32=w_up.astype(jnp.float32), w_down32=w_down.astype(jnp.float32)))
    routed = lax.map(block, (mixed.reshape(NUM_DEV, TOKENS, D), slot_ids.reshape(NUM_DEV, TOKENS, TOP), gate_vals.reshape(NUM_DEV, TOKENS, TOP)))
    routed = routed.reshape(ROWS, D)
    new_act = (mixed.astype(jnp.float32) + routed + shared_out).astype(jnp.bfloat16)
    return new_act, None


def reference(act_in, grad_out, slot_ids, gate_vals, w_dense, w_gate, w_up, w_down, ws_gate, ws_up, ws_down):
    def forward(act, dense_all, gate_all, up_all, down_all, sgate_all, sup_all, sdown_all):
        final, _ = lax.scan(moe_layer, act, (dense_all, gate_all, up_all, down_all, sgate_all, sup_all, sdown_all, slot_ids, gate_vals))
        return final
    _, pullback = jax.vjp(forward, act_in, w_dense, w_gate, w_up, w_down, ws_gate, ws_up, ws_down)
    grads = pullback(grad_out)
    return (grads[0], grads[1], grads[2], grads[3], grads[4], grads[5], grads[6], grads[7])
```

```python
import functools

import jax
import jax.numpy as jnp
from jax import lax
from jax.experimental import pallas as pl
from jax.experimental.pallas import tpu as pltpu
from jax.sharding import PartitionSpec as P

ALL_AXES = ("ep", "dp")
BF = jnp.bfloat16
F32 = jnp.float32
VMEM_LIMIT = 60 * 1024 * 1024


def silu_grad(pre_act):
    sigma = jax.nn.sigmoid(pre_act)
    return sigma * (1.0 + pre_act * (1.0 - sigma))


def contract_rows(left, right):
    return lax.dot_general(left, right, (((0,), (0,)), ((), ())), preferred_element_type=F32)


def contract_cols(left, right):
    return lax.dot_general(left, right, (((1,), (1,)), ((), ())), preferred_element_type=F32)


def pad_lanes(size):
    return (size + 127) // 128 * 128


def one_hot(row, count):
    ids = lax.broadcasted_iota(jnp.int32, (count, row.shape[-1]), 0)
    return ids == row


def as_bf16(mask):
    return jnp.where(mask, 1.0, 0.0).astype(BF)


def load_weights(first, w1_ref, w3_ref, w2_ref, w13, w2p):
    ff = w1_ref.shape[2]
    fp = w2p.shape[0]

    @pl.when(first)
    def _():
        w13[...] = jnp.zeros_like(w13)
        w2p[...] = jnp.zeros_like(w2p)

    w13[:, 0:ff] = w1_ref[0]
    w13[:, fp:fp + ff] = w3_ref[0]
    w2p[0:ff, :] = w2_ref[0]


def fwd_kernel(cap, group, rt_ref, gt_ref, u_ref, w1_ref, w3_ref, w2_ref, y_ref, w13, w2p, xs, go):
    expert = pl.program_id(0)
    sources, tokens, width = u_ref.shape
    fp = w2p.shape[0]
    load_weights(expert == 0, w1_ref, w3_ref, w2_ref, w13, w2p)

    @pl.when(expert == 0)
    def _():
        y_ref[...] = jnp.zeros_like(y_ref)

    slot = lax.rem(expert, group)

    @pl.loop(0, sources)
    def _(s):
        mask = one_hot(rt_ref[expert, s], cap)
        x = jnp.dot(as_bf16(mask), u_ref[s], preferred_element_type=F32).astype(BF)
        gate = jnp.sum(jnp.where(mask, gt_ref[expert, s], 0.0), axis=1, keepdims=True)
        a = jnp.dot(x, w13[...], preferred_element_type=F32)
        a1 = a[:, 0:fp]
        a3 = a[:, fp:2 * fp]
        h = (jax.nn.silu(a1) * a3).astype(BF)
        o = jnp.dot(h, w2p[...], preferred_element_type=F32).astype(BF)
        p = o.astype(F32) * gate
        hi = p.astype(BF)
        rest = p - hi.astype(F32)
        mid = rest.astype(BF)
        low = (rest - mid.astype(F32)).astype(BF)
        rows = pl.ds(pl.multiple_of(slot * cap, 16), cap)
        go[s, rows, 0:width] = hi
        go[s, rows, width:2 * width] = mid
        go[s, rows, 2 * width:3 * width] = low

    @pl.when(slot == group - 1)
    def _():
        tile = 256

        @pl.loop(0, sources * (tokens // tile))
        def _(step):
            s = step // (tokens // tile)
            at = pl.ds(pl.multiple_of(lax.rem(step, tokens // tile) * tile, tile), tile)
            hot = jnp.concatenate([as_bf16(one_hot(rt_ref[expert - (group - 1) + k, s, :, at], cap)) for k in range(group)], axis=0)
            d = contract_rows(hot, go[s])
            y_ref[s, at, :] += d[:, 0:width] + (d[:, width:2 * width] + d[:, 2 * width:3 * width])


def bwd_kernel(cap, count, has_acc, base_ref, rt_ref, gt_ref, u_ref, dy_ref, w1_ref, w3_ref, w2_ref, *rest):
    if has_acc:
        acc_ref, *rest = rest
    g1_ref, g3_ref, g2_ref, du_ref, w13, w2p, xs, ds, hs, das, dxs, hots = rest
    step = pl.program_id(0)
    sources, tokens, width = u_ref.shape
    ff = w1_ref.shape[2]
    fp = w2p.shape[0]

    @pl.when(step < count)
    def _():
        expert = base_ref[0] + step
        load_weights(step == 0, w1_ref, w3_ref, w2_ref, w13, w2p)

        @pl.loop(0, sources)
        def _(s):
            mask = one_hot(rt_ref[expert, s], cap)
            hot = as_bf16(mask)
            gate = jnp.sum(jnp.where(mask, gt_ref[expert, s], 0.0), axis=1, keepdims=True)
            rows = pl.ds(pl.multiple_of(s * cap, 16), cap)
            xs[rows, :] = jnp.dot(hot, u_ref[s], preferred_element_type=F32).astype(BF)
            ds[rows, :] = (jnp.dot(hot, dy_ref[s], preferred_element_type=F32) * gate).astype(BF)

        @pl.loop(0, sources // 2)
        def _(c):
            rows = pl.ds(pl.multiple_of(c * 2 * cap, 16), 2 * cap)
            a = jnp.dot(xs[rows, :], w13[...], preferred_element_type=F32)
            dh = contract_cols(ds[rows, :], w2p[...])
            a1 = a[:, 0:fp]
            a3 = a[:, fp:2 * fp]
            sigma = jax.nn.sigmoid(a1)
            si = a1 * sigma
            hs[rows, :] = (si * a3).astype(BF)
            das[rows, 0:fp] = (dh * a3 * (sigma * (1.0 + a1 * (1.0 - sigma)))).astype(BF)
            das[rows, fp:2 * fp] = (dh * si).astype(BF)
            dx = contract_cols(das[rows, :], w13[...]).astype(BF)
            into = pl.ds(pl.multiple_of(step * cap, 16), cap)
            dxs[2 * c, into, :] = dx[0:cap]
            dxs[2 * c + 1, into, :] = dx[cap:2 * cap]

        g2 = contract_rows(hs[...], ds[...])
        g2_ref[0] = g2[0:ff].astype(BF)
        g1 = contract_rows(xs[...], das[:, 0:fp])
        g1_ref[0] = g1[:, 0:ff].astype(BF)
        g3 = contract_rows(xs[...], das[:, fp:2 * fp])
        g3_ref[0] = g3[:, 0:ff].astype(BF)

    @pl.when(step >= count)
    def _():
        tile = hots.shape[1]
        s = step - count

        @pl.loop(0, tokens // tile)
        def _(t):
            at = pl.ds(pl.multiple_of(t * tile, tile), tile)
            for k in range(count):
                hots[k * cap:(k + 1) * cap, :] = as_bf16(one_hot(rt_ref[base_ref[0] + k, s, :, at], cap))
            d = contract_rows(hots[...], dxs[s])
            if has_acc:
                d = d + acc_ref[0, at, :]
            du_ref[0, at, :] = d.astype(du_ref.dtype)


def full_spec(shape):
    return pl.BlockSpec(shape, lambda *_: (0,) * len(shape), pipeline_mode=pl.Buffered(1))


def experts_forward(rt, gt, u, w_gate, w_up, w_down, cap):
    experts, width, ff = w_gate.shape
    sources, tokens, _ = u.shape
    fp = pad_lanes(ff)
    group = 4
    rows = experts * sources * cap
    spec = lambda a, b: pl.BlockSpec((1, a, b), lambda e: (e, 0, 0))
    return pl.pallas_call(
        functools.partial(fwd_kernel, cap, group),
        out_shape=jax.ShapeDtypeStruct((sources, tokens, width), F32),
        grid=(experts,),
        in_specs=[full_spec(rt.shape), full_spec(gt.shape), full_spec(u.shape), spec(width, ff), spec(width, ff), spec(ff, width)],
        out_specs=full_spec((sources, tokens, width)),
        scratch_shapes=[
            pltpu.VMEM((width, 2 * fp), BF),
            pltpu.VMEM((fp, width), BF),
            pltpu.VMEM((8, 128), BF),
            pltpu.VMEM((sources, group * cap, 3 * width), BF),
        ],
        compiler_params=pltpu.CompilerParams(vmem_limit_bytes=VMEM_LIMIT),
        cost_estimate=pl.CostEstimate(flops=2 * rows * width * (4 * tokens + 3 * ff), bytes_accessed=experts * 3 * width * ff * 2 + u.size * 6, transcendentals=0),
        name="experts_forward",
    )(rt, gt, u, w_gate, w_up, w_down)


def experts_backward(base, count, rt, gt, u, dy, w_gate, w_up, w_down, cap, acc):
    _, width, ff = w_gate.shape
    sources, tokens, _ = u.shape
    fp = pad_lanes(ff)
    has_acc = acc is not None
    rows = count * sources * cap
    last = count - 1
    win = lambda a, b: pl.BlockSpec((1, a, b), lambda i, base_ref: (base_ref[0] + jnp.minimum(i, last), 0, 0))
    wout = lambda a, b: pl.BlockSpec((1, a, b), lambda i, base_ref: (jnp.minimum(i, last), 0, 0))
    part = pl.BlockSpec((1, tokens, width), lambda i, base_ref: (jnp.maximum(i - count, 0), 0, 0))
    in_specs = [full_spec(rt.shape), full_spec(gt.shape), full_spec(u.shape), full_spec(dy.shape), win(width, ff), win(width, ff), win(ff, width)]
    args = [rt, gt, u, dy, w_gate, w_up, w_down]
    if has_acc:
        in_specs.append(part)
        args.append(acc)
    return pl.pallas_call(
        functools.partial(bwd_kernel, cap, count, has_acc),
        out_shape=(
            jax.ShapeDtypeStruct((count, width, ff), BF),
            jax.ShapeDtypeStruct((count, width, ff), BF),
            jax.ShapeDtypeStruct((count, ff, width), BF),
            jax.ShapeDtypeStruct((sources, tokens, width), BF if has_acc else F32),
        ),
        grid_spec=pltpu.PrefetchScalarGridSpec(
            num_scalar_prefetch=1,
            grid=(count + sources,),
            in_specs=in_specs,
            out_specs=(wout(width, ff), wout(width, ff), wout(ff, width), part),
            scratch_shapes=[
                pltpu.VMEM((width, 2 * fp), BF),
                pltpu.VMEM((fp, width), BF),
                pltpu.VMEM((sources * cap, width), BF),
                pltpu.VMEM((sources * cap, width), BF),
                pltpu.VMEM((sources * cap, fp), BF),
                pltpu.VMEM((sources * cap, 2 * fp), BF),
                pltpu.VMEM((sources, count * cap, width), BF),
                pltpu.VMEM((count * cap, 256), BF),
            ],
        ),
        compiler_params=pltpu.CompilerParams(vmem_limit_bytes=VMEM_LIMIT),
        cost_estimate=pl.CostEstimate(flops=2 * rows * width * (3 * tokens + 8 * ff), bytes_accessed=count * 6 * width * ff * 2 + u.size * 6, transcendentals=0),
        name="experts_backward",
    )(base, *args)


def solution(mesh):
    ep_size = mesh.shape["ep"]
    dp_size = mesh.shape["dp"]
    tok_spec = P(ALL_AXES, None)
    route_spec = P(None, ALL_AXES, None)
    exp_spec = P(None, "ep", None, None)
    repl_spec = P(None, None, None)
    core_perm = [(i, i ^ 1) for i in range(dp_size)]
    x_perm = [(i, i ^ 2) for i in range(dp_size)]

    def to_f32(value):
        return value.astype(F32)

    def gather_ep(value):
        return lax.all_gather(value, "ep", axis=0)

    def sum_home(parts):
        back = lax.all_to_all(parts, "ep", 0, 0)
        return jnp.sum(to_f32(back), axis=0)

    def reduce_experts(theirs, mine):
        mine = [(to_f32(m) + to_f32(lax.ppermute(t, "dp", core_perm))).astype(BF) for t, m in zip(theirs, mine)]
        total = [(to_f32(m) + to_f32(lax.ppermute(m, "dp", x_perm))).astype(BF) for m in mine]
        other = [lax.ppermute(t, "dp", core_perm) for t in total]
        return total, other

    def body(act_in, grad_out, slot_ids, gate_vals, w_dense, w_gate, w_up, w_down, ws_gate, ws_up, ws_down):
        layers = w_dense.shape[0]
        tokens, width = act_in.shape
        top = slot_ids.shape[2]
        experts = w_gate.shape[1]
        half = experts // 2
        cap = 2 * tokens * top // (experts * ep_size)
        core = lax.rem(lax.axis_index("dp"), 2)
        first = experts * lax.axis_index("ep")

        meta = jnp.concatenate([slot_ids.astype(F32), gate_vals], axis=2).transpose(0, 2, 1)
        meta = gather_ep(meta)
        slots = meta[:, :, 0:top].astype(jnp.int32).transpose(1, 0, 2, 3)[:, None]
        gates = meta[:, :, top:].transpose(1, 0, 2, 3)[:, None]
        ids = first + lax.broadcasted_iota(jnp.int32, (1, experts, 1, 1, 1), 1)
        match = slots // cap == ids
        rt_all = jnp.max(jnp.where(match, slots % cap, -1), axis=3)[:, :, :, None]
        gt_all = jnp.sum(jnp.where(match, gates, 0.0), axis=3)[:, :, :, None]

        acts = [act_in]
        mixed = []
        mixed_all = []
        grad_out_all = gather_ep(grad_out)
        for layer in range(layers):
            act = acts[layer]
            u = (to_f32(act) + jnp.dot(act, w_dense[layer], preferred_element_type=F32)).astype(BF)
            mixed.append(u)
            mixed_all.append(gather_ep(u))
            if layer + 1 < layers:
                parts = experts_forward(rt_all[layer], gt_all[layer], mixed_all[layer], w_gate[layer], w_up[layer], w_down[layer], cap)
                s_one = jnp.dot(u, ws_gate[layer], preferred_element_type=F32)
                s_three = jnp.dot(u, ws_up[layer], preferred_element_type=F32)
                shared_hidden = (jax.nn.silu(s_one) * s_three).astype(BF)
                shared_out = jnp.dot(shared_hidden, ws_down[layer], preferred_element_type=F32)
                acts.append((to_f32(u) + sum_home(parts) + shared_out).astype(BF))

        grad_y = grad_out
        dense_sums = [None] * layers
        expert_sums = [None] * layers
        for layer in reversed(range(layers)):
            u = mixed[layer]
            grad_all = grad_out_all if layer + 1 == layers else gather_ep(grad_y)
            call = lambda base, acc: experts_backward(
                base.reshape(1), half, rt_all[layer], gt_all[layer], mixed_all[layer], grad_all,
                w_gate[layer], w_up[layer], w_down[layer], cap, acc)
            *theirs, acc = call(half * (1 - core), None)
            *own, parts = call(half * core, acc)
            expert_sums[layer] = reduce_experts(theirs, own)

            s_one = jnp.dot(u, ws_gate[layer], preferred_element_type=F32)
            s_three = jnp.dot(u, ws_up[layer], preferred_element_type=F32)
            shared_hidden = (jax.nn.silu(s_one) * s_three).astype(BF)
            g_ws_down = contract_rows(shared_hidden, grad_y)
            grad_shared = contract_cols(grad_y, ws_down[layer])
            grad_s_one = (grad_shared * s_three * silu_grad(s_one)).astype(BF)
            grad_s_three = (grad_shared * jax.nn.silu(s_one)).astype(BF)
            g_ws_gate = contract_rows(u, grad_s_one)
            g_ws_up = contract_rows(u, grad_s_three)
            grad_mixed = (to_f32(grad_y) + sum_home(parts) + contract_cols(grad_s_one, ws_gate[layer]) + contract_cols(grad_s_three, ws_up[layer])).astype(BF)
            g_w_dense = contract_rows(acts[layer], grad_mixed)
            grad_y = (to_f32(grad_mixed) + contract_cols(grad_mixed, w_dense[layer])).astype(BF)
            dense = tuple(g.astype(BF) for g in (g_w_dense, g_ws_gate, g_ws_up, g_ws_down))
            if layer + 1 < layers:
                dense, later = lax.optimization_barrier((dense, dense_sums[layer + 1]))
                dense_sums[layer + 1] = later
            dense_sums[layer] = tuple(lax.psum(g, ALL_AXES) for g in dense)

        dense_out = [jnp.stack([dense_sums[layer][which] for layer in range(layers)]) for which in range(4)]
        expert_out = []
        for which in range(3):
            total = jnp.stack([expert_sums[layer][0][which] for layer in range(layers)])
            other = jnp.stack([expert_sums[layer][1][which] for layer in range(layers)])
            expert_out.append(jnp.where(core == 0, jnp.concatenate([total, other], axis=1), jnp.concatenate([other, total], axis=1)))
        return (grad_y, dense_out[0], expert_out[0], expert_out[1], expert_out[2], dense_out[1], dense_out[2], dense_out[3])

    return jax.shard_map(body, mesh=mesh, in_specs=(tok_spec, tok_spec, route_spec, route_spec, repl_spec, exp_spec, exp_spec, exp_spec, repl_spec, repl_spec, repl_spec), out_specs=(tok_spec, repl_spec, exp_spec, exp_spec, exp_spec, repl_spec, repl_spec, repl_spec), check_vma=False)
```
